256 devices in a mesh: dp: 8 (over x, core), expert: 32 (over z, y).
Axes of the slice: x: 4, y: 4, z: 8, core: 2. Of those that a mesh axis runs over, the one named last changes fastest.
Arguments:
- tokens: bfloat16 [2048, 6144], P('dp', 'expert'), may hold values from -6 to 6
- cotangent: bfloat16 [2048, 6144], P('dp', 'expert'), may hold values from -6 to 6
- expert_choice: int32 [2048, 2], P('dp'), may hold values from 0 to 7, all different within a row; in each aligned block of 256 rows (0 to 255, 256 to 511, ...) at most 80 rows name the same one
- gate_values: bfloat16 [2048, 2], P('dp'), may hold values from 0.099609375 to 1
- gate_weight: bfloat16 [8, 6144, 8192], P('dp', None, 'expert'), may hold values from -0.078125 to 0.078125
- up_weight: bfloat16 [8, 6144, 8192], P('dp', None, 'expert'), may hold values from -0.078125 to 0.078125
- down_weight: bfloat16 [8, 8192, 6144], P('dp', 'expert'), may hold values from -0.0625 to 0.0625
- shrinker: bfloat16 [8, 32, 6144], P('dp'), may hold values from -0.078125 to 0.078125
- widener: bfloat16 [8, 2, 16, 8192], P('dp', None, None, 'expert'), may hold values from -0.375 to 0.375
- squeezer: bfloat16 [8, 16, 8192], P('dp', None, 'expert'), may hold values from -0.0625 to 0.0625
- spreader: bfloat16 [8, 16, 6144], P('dp'), may hold values from -0.375 to 0.375
Outputs:
- token_grad: bfloat16 [2048, 6144], P('dp', 'expert')
- gate_grad: float32 [2048, 2], P('dp')
- shrinker_grad: float32 [8, 32, 6144], P('dp')
- widener_grad: float32 [8, 2, 16, 8192], P('dp', None, None, 'expert')
- squeezer_grad: float32 [8, 16, 8192], P('dp', None, 'expert')
- spreader_grad: float32 [8, 16, 6144], P('dp')
The draws below stay inside these ranges and needn't reach their ends.
Inputs may be any that keep to these rules, and one draw needn't show every extreme that they name: `expert_choice`: each row names 2 different experts. Among the 256 tokens of one index of dp no expert is chosen more than 80 times, and some expert is chosen exactly 80 times by the tokens of some or all indices of dp.
All inputs are finite; a program needn't handle non-finite values.
Results may differ from the reference program's by a relative error of at most 0.02.
Values may be sent and summed in bfloat16 or wider, within the bound.
No kernel may reach another device: no remote copies, remote signals or barrier semaphores. Data moves between devices by JAX's collectives and lax.ppermute only.
A program may use at most 128 MiB of HBM per device.

```python
import math
import jax
import jax.numpy as jnp
import numpy as np
from jax import lax

D = 6144
EXPERTS = 8
FF = 8192
RANK = 16
TOP = 2
TOK_DEV = 256
TOKENS = 2048
CAP = 80
N_DP = 8
N_EXPERT = 32


def steps_of(rng, extent, split, least, top_value):
    def one(dim, parts):
        steps = jax.random.uniform(jax.random.fold_in(jax.random.fold_in(rng, 6), dim), (parts,), jnp.float32, least / len(split), top_value / len(split))
        return jnp.repeat(jnp.exp(steps), extent[dim] // parts).reshape((-1,) + (1,) * (len(extent) - dim - 1))

    gain = one(*split[0])
    for cut in split[1:]:
        gain = gain * one(*cut)
    return gain


def shared_out(stream_key, own, number, rows, amount, top, bound, slope):
    ranking = jax.random.permutation(stream_key, amount)
    crowded, common = shares(amount, rows * top, bound, slope, True), shares(amount, rows * top, bound, slope, False)
    places = jnp.arange(amount)

    def named(sizes, rotation):
        used = int((sizes > 0).sum())
        fixed = max(1, used // 4)
        shifted = fixed + (places - fixed + rotation * (used - fixed)) % max(1, amount - fixed)
        return jnp.zeros((amount,), jnp.int32).at[ranking[jnp.where(places < fixed, places, shifted)]].set(jnp.asarray(sizes, jnp.int32))

    sizes = jnp.where(number % 4 == 0, named(crowded, number // 4), named(common, number - number // 4 - 1))
    mixed = jax.random.permutation(jax.random.fold_in(own, 3), amount)
    donor, receiver = mixed[0:amount // 2 * 2:2], mixed[1:amount // 2 * 2:2]
    slack = jnp.minimum(sizes[donor] - 1, bound - sizes[receiver]) // 2
    slack = jnp.where((donor == ranking[0]) | (receiver == ranking[0]) | (sizes[receiver] == 0), 0, jnp.maximum(slack, 0))
    shifted = jax.random.randint(jax.random.fold_in(own, 4), (amount // 2,), 0, 1 << 20) % (slack + 1)
    sizes = sizes.at[donor].add(-shifted).at[receiver].add(shifted)
    labels = jnp.searchsorted(jnp.cumsum(sizes), jnp.arange(rows * top), side="right").astype(jnp.int32)
    grid = labels.reshape(top, rows).T
    grid = grid[jax.random.permutation(jax.random.fold_in(own, 1), rows)]
    rotation = jax.random.randint(jax.random.fold_in(own, 2), (rows, 1), 0, top)
    return jnp.take_along_axis(grid, (jnp.arange(top)[None, :] + rotation) % top, axis=1)


def shares(count, total, most, slope, full):
    weights = [(1 << 20) // math.isqrt(standing ** slope) + 1 for standing in range(1, count + 1)]
    largest = most if full else min(most, max(-(-total // count), total * weights[0] // sum(weights)))
    least = 1 if total - largest >= count - 1 else 0
    holding, surplus = [largest] + [least] * (count - 1), total - largest - least * (count - 1)
    while surplus > 0:
        candidates = [i for i in range(1, count) if holding[i] < largest] or [i for i in range(1, count) if holding[i] < most]
        whole, budget = sum([weights[i] for i in candidates]), surplus
        for i in candidates:
            addition = min(most - holding[i], max(1, budget * weights[i] // whole), surplus)
            holding[i] = holding[i] + addition
            surplus = surplus - addition
    return np.array(holding)


def bell_draw(own_key, extent, spread, limit, split=(), kind=jnp.bfloat16):
    loudness = steps_of(own_key, extent, split, -0.22, 0.18) if split else 1.0
    drawn = jax.random.normal(own_key, extent, jnp.float32) * spread * loudness
    return jnp.minimum(jnp.maximum(drawn, -limit), limit).astype(kind)


def setup_inputs(seed: int = 0) -> dict:
    key_of = jax.random.split(jax.random.key(seed), 12)
    tokens = bell_draw(key_of[0], (TOKENS, D), 1.0, 6.0, ((0, 8), (1, 32)))
    cotangent = bell_draw(key_of[1], (TOKENS, D), 1.0, 6.0, ((0, 8), (1, 32)))
    expert_choice_keys = jax.random.split(jax.random.fold_in(key_of[2], 1), TOKENS // TOK_DEV)
    expert_choice_turns = jax.random.permutation(jax.random.fold_in(key_of[2], 3), TOKENS // TOK_DEV)
    expert_choice = jax.vmap(lambda own, number: shared_out(jax.random.fold_in(key_of[2], 2), own, number, TOK_DEV, EXPERTS, TOP, CAP, 2))(expert_choice_keys, expert_choice_turns).reshape((TOKENS, TOP))
    gate_values = jnp.clip(0.099609375 + 0.9003906 * jax.random.uniform(key_of[3], (TOKENS, TOP), jnp.float32) ** steps_of(key_of[3], (TOKENS, TOP), ((0, 8),), -0.2, 0.2), 0.099609375, 1.0).astype(jnp.bfloat16)
    gate_weight = bell_draw(key_of[4], (EXPERTS, D, FF), D ** -0.5, 0.078125, ((0, 8), (2, 32)))
    up_weight = bell_draw(key_of[5], (EXPERTS, D, FF), D ** -0.5, 0.078125, ((0, 8), (2, 32)))
    down_weight = bell_draw(key_of[6], (EXPERTS, FF, D), FF ** -0.5, 0.0625, ((0, 8), (1, 32)))
    shrinker = bell_draw(key_of[7], (EXPERTS, 2 * RANK, D), D ** -0.5, 0.078125, ((0, 8),))
    widener = bell_draw(key_of[8], (EXPERTS, 2, RANK, FF), (16 * RANK) ** -0.5, 0.375, ((0, 8), (3, 32)))
    squeezer = bell_draw(key_of[9], (EXPERTS, RANK, FF), FF ** -0.5, 0.0625, ((0, 8), (2, 32)))
    spreader = bell_draw(key_of[10], (EXPERTS, RANK, D), (16 * RANK) ** -0.5, 0.375, ((0, 8),))
    return dict(tokens=tokens, cotangent=cotangent, expert_choice=expert_choice, gate_values=gate_values, gate_weight=gate_weight, up_weight=up_weight, down_weight=down_weight, shrinker=shrinker, widener=widener, squeezer=squeezer, spreader=spreader)


adapter_scale = 2.0


def matmul(operand_a, operand_b):
    return jnp.dot(operand_a, operand_b, preferred_element_type=jnp.float32)


def silu_pair(gate_pre):
    logistic = jax.nn.sigmoid(gate_pre)
    return gate_pre * logistic, logistic * (1.0 + gate_pre * (1.0 - logistic))


def blockwise_grads(gate_delta, up_delta, gate_matrix, up_matrix):
    row_count = gate_delta.shape[0]
    ff_block = FF // N_EXPERT
    gate_parts = jnp.einsum("nkf,dkf->knd", gate_delta.astype(jnp.float32).reshape(row_count, N_EXPERT, ff_block), gate_matrix.astype(jnp.float32).reshape(D, N_EXPERT, ff_block))
    up_parts = jnp.einsum("nkf,dkf->knd", up_delta.astype(jnp.float32).reshape(row_count, N_EXPERT, ff_block), up_matrix.astype(jnp.float32).reshape(D, N_EXPERT, ff_block))
    rounded = lax.optimization_barrier((gate_parts + up_parts).astype(jnp.bfloat16))
    return jnp.sum(rounded.astype(jnp.float32), axis=0)


def reference(tokens, cotangent, expert_choice, gate_values, gate_weight, up_weight, down_weight, shrinker, widener, squeezer, spreader):
    blocks = N_DP
    per_block = TOK_DEV * TOP
    route_rows = expert_choice.reshape(blocks, per_block).astype(jnp.int32)
    onehot = (route_rows[:, :, None] == jnp.arange(EXPERTS, dtype=jnp.int32)[None, None, :]).astype(jnp.int32)
    before = (jnp.cumsum(onehot, axis=1) - onehot).astype(jnp.int32)
    slot_index = jnp.sum(before * onehot, axis=2).astype(jnp.int32)
    stacked = jnp.concatenate([tokens, cotangent], axis=1).astype(jnp.float32)
    stacked = jnp.repeat(stacked, TOP, axis=0).reshape(blocks, per_block, 2 * D)
    gate_rows = gate_values.reshape(blocks, per_block).astype(jnp.float32)
    slot_range = jnp.arange(CAP, dtype=jnp.int32)

    def per_expert(expert):
        chosen = ((route_rows[:, None, :] == expert) & (slot_index[:, None, :] == slot_range[None, :, None])).astype(jnp.float32)
        picked = jnp.einsum("bcj,bjd->bcd", chosen, stacked).reshape(blocks * CAP, 2 * D).astype(jnp.bfloat16)
        rows_x = picked[:, :D]
        rows_dy = picked[:, D:]
        rows_gate = jnp.sum(chosen * gate_rows[:, None, :], axis=2).reshape(blocks * CAP)
        lowrank_in = matmul(rows_x, shrinker[expert].T).astype(jnp.bfloat16)
        gate_pre = matmul(rows_x, gate_weight[expert]) + adapter_scale * matmul(lowrank_in[:, :RANK], widener[expert, 0])
        up_pre = matmul(rows_x, up_weight[expert]) + adapter_scale * matmul(lowrank_in[:, RANK:], widener[expert, 1])
        silu_gate, silu_slope = silu_pair(gate_pre)
        activation = (silu_gate * up_pre).astype(jnp.bfloat16)
        out_low = matmul(activation, squeezer[expert].T)
        low_out = out_low.astype(jnp.bfloat16)
        back_down = matmul(rows_dy, down_weight[expert].T)
        back_low = matmul(rows_dy, spreader[expert].T)
        gate_dots = jnp.sum(activation.astype(jnp.float32) * back_down, axis=1) + adapter_scale * jnp.sum(low_out.astype(jnp.float32) * back_low, axis=1)
        scaled_low = (rows_gate[:, None] * back_low).astype(jnp.bfloat16)
        act_delta = rows_gate[:, None] * back_down + adapter_scale * matmul(scaled_low, squeezer[expert])
        gate_delta = (act_delta * up_pre * silu_slope).astype(jnp.bfloat16)
        up_delta = (act_delta * silu_gate).astype(jnp.bfloat16)
        back_in = jnp.concatenate([matmul(gate_delta, widener[expert, 0].T), matmul(up_delta, widener[expert, 1].T)], axis=1).astype(jnp.bfloat16)
        row_grads = blockwise_grads(gate_delta, up_delta, gate_weight[expert], up_weight[expert]) + adapter_scale * matmul(back_in, shrinker[expert])
        shrink_grad = adapter_scale * matmul(back_in.T, rows_x)
        widen_grad = adapter_scale * jnp.stack([matmul(lowrank_in[:, :RANK].T, gate_delta), matmul(lowrank_in[:, RANK:].T, up_delta)])
        squeeze_grad = adapter_scale * matmul(scaled_low.T, activation)
        weighted_low = (rows_gate[:, None] * out_low).astype(jnp.bfloat16)
        spread_grad = adapter_scale * matmul(weighted_low.T, rows_dy)
        return row_grads, gate_dots, shrink_grad, widen_grad, squeeze_grad, spread_grad

    results = lax.map(per_expert, jnp.arange(EXPERTS, dtype=jnp.int32))
    row_grads, gate_dots, shrinker_grad, widener_grad, squeezer_grad, spreader_grad = results
    block_base = (jnp.arange(blocks, dtype=jnp.int32) * CAP)[:, None]
    position = (route_rows * (blocks * CAP) + block_base + slot_index).reshape(-1).astype(jnp.int32)
    picked_rows = jnp.take(row_grads.reshape(EXPERTS * blocks * CAP, D), position, axis=0)
    token_grad = jnp.sum(picked_rows.reshape(TOKENS, TOP, D), axis=1).astype(jnp.bfloat16)
    gate_grad = jnp.take(gate_dots.reshape(-1), position).reshape(TOKENS, TOP)
    return token_grad, gate_grad, shrinker_grad, widener_grad, squeezer_grad, spreader_grad
```

```python
import jax
import jax.numpy as jnp
from jax import lax
from jax.experimental import pallas as pl
from jax.experimental.pallas import tpu as pltpu
from jax.sharding import PartitionSpec as P


adapter_scale = 2.0
NY = 4
NZ = 8
GATE_ROWS = 8
BACK_WIDTH = 256
SPLIT_ROWS = 96

bf16 = jnp.bfloat16
f32 = jnp.float32


def dot(a, b, dims):
    return lax.dot_general(a, b, (dims, ((), ())), preferred_element_type=f32)


def shift_y(x, d):
    pairs = [(z * NY + y, z * NY + (y + d) % NY) for z in range(NZ) for y in range(NY)]
    return lax.ppermute(x, "expert", pairs)


def shift_z(x, d):
    pairs = [(z * NY + y, (z + d) % NZ * NY + y) for z in range(NZ) for y in range(NY)]
    return lax.ppermute(x, "expert", pairs)


def far_pair(up, down, shift):
    half = up.shape[-2] // 32 * 16
    return jnp.concatenate(
        [shift(up[..., :half, :], 1), shift(down[..., half:, :], -1)], axis=-2
    )


def ring_gather(x, n, shift):
    pieces = [(0, x)]
    up = down = x
    for step in range(1, n // 2):
        up, down = shift(up, 1), shift(down, -1)
        pieces += [(-step, up), (step, down)]
    pieces.append((n // 2, far_pair(up, down, shift)))
    return pieces


def ring_reduce(blocks, n, shift, seen=None):
    far = blocks(n // 2).astype(bf16)
    half = far.shape[-2] // 32 * 16
    up = shift(far[..., :half, :], 1)
    down = shift(far[..., half:, :], -1)
    if seen is not None:
        seen.append(up)
    lead = [(0, 0)] * (far.ndim - 2)
    rest = far.shape[-2] - half
    up = jnp.pad(up.astype(f32), lead + [(0, rest), (0, 0)])
    down = jnp.pad(down.astype(f32), lead + [(half, 0), (0, 0)])
    for k in range(n // 2 - 1, 0, -1):
        up = shift((up + blocks(k)).astype(bf16), 1)
        down = shift((down + blocks(-k)).astype(bf16), -1)
        if seen is not None:
            seen.append(up)
        up, down = up.astype(f32), down.astype(f32)
    return up + down + blocks(0)


def all_sum(x, after):
    for i, bit in enumerate((1, 2, 4, 8, 16)):
        pairs = [(e, e ^ bit) for e in range(NY * NZ)]
        x = x.astype(bf16)
        if 0 < i <= len(after):
            x, _ = lax.optimization_barrier((x, after[i - 1]))
        x = x.astype(f32) + lax.ppermute(x, "expert", pairs).astype(f32)
    return x


def turn_kernel(got_ref, first_ref, second_ref, rows_ref):
    n, _, cols = got_ref.shape
    capacity = rows_ref.shape[0] // n
    for b in range(n):
        rows_ref[b * capacity : (b + 1) * capacity, :] = got_ref[b, :capacity, :]
    turned = rows_ref[...].T
    first_ref[...] = turned[: cols // 2]
    second_ref[...] = turned[cols // 2 :]


def turn(got, capacity):
    n, _, cols = got.shape
    rows = n * capacity
    return pl.pallas_call(
        turn_kernel,
        out_shape=(
            jax.ShapeDtypeStruct((cols // 2, rows), bf16),
            jax.ShapeDtypeStruct((cols // 2, rows), bf16),
        ),
        scratch_shapes=[pltpu.VMEM((rows, cols), bf16)],
        name="turn",
    )(got)


SMALL = pl.BlockSpec(memory_space=pltpu.SMEM)
BIG = pl.BlockSpec(memory_space=pltpu.VMEM)


def x_products(place, x, gate_w_ref, up_w_ref, shrink_ref, accs, start):
    products = (
        dot(gate_w_ref[place], x, ((0,), (0,))),
        dot(up_w_ref[place], x, ((0,), (0,))),
        dot(shrink_ref[place], x, ((1,), (0,))),
    )
    for acc, value in zip(accs, products, strict=True):
        acc[...] = value if start else acc[...] + value


def dy_products(place, dy, down_w_ref, spread_ref, accs, start):
    products = (
        dot(down_w_ref[place], dy, ((1,), (0,))),
        dot(spread_ref[place], dy, ((1,), (0,))),
    )
    for acc, value in zip(accs, products, strict=True):
        acc[...] = value if start else acc[...] + value


def early_x(places, pieces, gate_w, up_w, shrink):
    def kernel(places_ref, gate_w_ref, up_w_ref, shrink_ref, *refs):
        piece_refs, accs = refs[: len(pieces)], refs[len(pieces) :]
        for i, ref in enumerate(piece_refs):
            x_products(places_ref[i], ref[...], gate_w_ref, up_w_ref, shrink_ref, accs, i == 0)

    hidden, n_rows = gate_w.shape[2], pieces[0].shape[1]
    return pl.pallas_call(
        kernel,
        in_specs=[SMALL] + [BIG] * (3 + len(pieces)),
        out_specs=[BIG] * 3,
        out_shape=[
            jax.ShapeDtypeStruct((hidden, n_rows), f32),
            jax.ShapeDtypeStruct((hidden, n_rows), f32),
            jax.ShapeDtypeStruct((shrink.shape[1], n_rows), f32),
        ],
        name="early_x",
    )(places, gate_w, up_w, shrink, *pieces)


def early_dy(places, pieces, down_w, spread):
    def kernel(places_ref, down_w_ref, spread_ref, *refs):
        piece_refs, accs = refs[: len(pieces)], refs[len(pieces) :]
        for i, ref in enumerate(piece_refs):
            dy_products(places_ref[i], ref[...], down_w_ref, spread_ref, accs, i == 0)

    hidden, n_rows = down_w.shape[1], pieces[0].shape[1]
    return pl.pallas_call(
        kernel,
        in_specs=[SMALL] + [BIG] * (2 + len(pieces)),
        out_specs=[BIG] * 2,
        out_shape=[
            jax.ShapeDtypeStruct((hidden, n_rows), f32),
            jax.ShapeDtypeStruct((spread.shape[1], n_rows), f32),
        ],
        name="early_dy",
    )(places, down_w, spread, *pieces)


def middle_kernel(
    places_ref,
    x_ref,
    dy_ref,
    gate_w_ref,
    up_w_ref,
    down_w_ref,
    shrink_ref,
    spread_ref,
    widen_ref,
    squeeze_ref,
    gates_ref,
    gate_in_ref,
    up_in_ref,
    low_in_ref,
    down_in_ref,
    spread_in_ref,
    deltas_ref,
    scaled_ref,
    back_low_ref,
    parts_ref,
    widen_grad_ref,
    squeeze_grad_ref,
):
    z, y = places_ref[0], places_ref[1]
    x, dy = x_ref[...], dy_ref[...]
    rank, hidden = squeeze_ref.shape
    n_rows = x.shape[1]
    gates = gates_ref[...]
    squeeze = squeeze_ref[...]
    low = (low_in_ref[...] + dot(shrink_ref[z], x, ((1,), (0,)))).astype(bf16)
    back_low = spread_in_ref[...] + dot(spread_ref[y], dy, ((1,), (0,)))
    back_low_ref[...] = back_low
    scaled = (back_low * gates).astype(bf16)
    scaled_ref[...] = scaled
    gate_pre = (
        gate_in_ref[...]
        + dot(gate_w_ref[z], x, ((0,), (0,)))
        + adapter_scale * dot(widen_ref[0], low[:rank], ((0,), (0,)))
    )
    up_pre = (
        up_in_ref[...]
        + dot(up_w_ref[z], x, ((0,), (0,)))
        + adapter_scale * dot(widen_ref[1], low[rank:], ((0,), (0,)))
    )
    back_down = down_in_ref[...] + dot(down_w_ref[y], dy, ((1,), (0,)))
    logistic = jax.nn.sigmoid(gate_pre)
    silu_gate = gate_pre * logistic
    activation = (silu_gate * up_pre).astype(bf16)
    gate_part = jnp.sum(activation.astype(f32) * back_down, axis=0, keepdims=True)
    act_delta = gates * back_down + adapter_scale * dot(squeeze, scaled, ((0,), (0,)))
    slope = logistic * (1.0 + gate_pre * (1.0 - logistic))
    gate_delta = (act_delta * up_pre * slope).astype(bf16)
    up_delta = (act_delta * silu_gate).astype(bf16)
    deltas_ref[:hidden, :] = gate_delta
    deltas_ref[hidden:, :] = up_delta
    parts_ref[:rank, :] = dot(widen_ref[0], gate_delta, ((1,), (0,))).astype(bf16)
    parts_ref[rank : 2 * rank, :] = dot(widen_ref[1], up_delta, ((1,), (0,))).astype(bf16)
    parts_ref[2 * rank : 3 * rank, :] = dot(squeeze, activation, ((1,), (0,))).astype(bf16)
    parts_ref[3 * rank :, :] = jnp.broadcast_to(gate_part, (rank, n_rows)).astype(bf16)
    widen_grad_ref[0] = adapter_scale * dot(low[:rank], gate_delta, ((1,), (1,)))
    widen_grad_ref[1] = adapter_scale * dot(low[rank:], up_delta, ((1,), (1,)))
    squeeze_grad_ref[...] = adapter_scale * dot(scaled, activation, ((1,), (1,)))


def middle(places, x, dy, gate_w, up_w, down_w, shrink, spread, widen, squeeze, gates, *sums):
    rank, hidden = squeeze.shape
    n_rows = x.shape[1]
    return pl.pallas_call(
        middle_kernel,
        in_specs=[SMALL] + [BIG] * 15,
        out_specs=[BIG] * 6,
        out_shape=[
            jax.ShapeDtypeStruct((2 * hidden, n_rows), bf16),
            jax.ShapeDtypeStruct((rank, n_rows), bf16),
            jax.ShapeDtypeStruct((rank, n_rows), f32),
            jax.ShapeDtypeStruct((4 * rank, n_rows), bf16),
            jax.ShapeDtypeStruct((2, rank, hidden), f32),
            jax.ShapeDtypeStruct((rank, hidden), f32),
        ],
        name="middle",
    )(places, x, dy, gate_w, up_w, down_w, shrink, spread, widen, squeeze, gates, *sums)


def term_kernel(gate_w_ref, up_w_ref, deltas_ref, out_ref):
    blocks, part, hidden = gate_w_ref.shape
    weights = jnp.concatenate(
        [
            gate_w_ref[...].reshape(blocks * part, hidden),
            up_w_ref[...].reshape(blocks * part, hidden),
        ],
        axis=1,
    )
    total = dot(weights, deltas_ref[...], ((1,), (0,)))
    out_ref[...] = total.astype(bf16).reshape(out_ref.shape)


def input_term(gate_w, up_w, deltas, part):
    n_blocks, width, hidden = gate_w.shape
    n_rows = deltas.shape[1]
    per = 8
    return pl.pallas_call(
        term_kernel,
        grid=(n_blocks // per,),
        in_specs=[
            pl.BlockSpec((per, SPLIT_ROWS, hidden), lambda i: (i, part, 0)),
            pl.BlockSpec((per, SPLIT_ROWS, hidden), lambda i: (i, part, 0)),
            pl.BlockSpec((2 * hidden, n_rows), lambda i: (0, 0)),
        ],
        out_specs=pl.BlockSpec((per, SPLIT_ROWS, n_rows), lambda i: (i, 0, 0)),
        out_shape=jax.ShapeDtypeStruct((n_blocks, SPLIT_ROWS, n_rows), bf16),
        name="input_term",
    )(gate_w, up_w, deltas)


def adapter_grads(places, x_pieces, dy_pieces, back_in, weighted):
    n_x, n_dy = len(x_pieces), len(dy_pieces)

    def kernel(places_ref, back_in_ref, weighted_ref, *refs):
        shrink_ref, spread_ref = refs[n_x + n_dy :]
        for i in range(n_x):
            shrink_ref[places_ref[i]] = adapter_scale * dot(back_in_ref[...], refs[i][...], ((1,), (1,)))
        for i in range(n_dy):
            spread_ref[places_ref[n_x + i]] = adapter_scale * dot(
                weighted_ref[...], refs[n_x + i][...], ((1,), (1,))
            )

    return pl.pallas_call(
        kernel,
        in_specs=[SMALL] + [BIG] * (2 + n_x + n_dy),
        out_specs=[BIG] * 2,
        out_shape=[
            jax.ShapeDtypeStruct((n_x, back_in.shape[0], x_pieces[0].shape[0]), f32),
            jax.ShapeDtypeStruct((n_dy, weighted.shape[0], dy_pieces[0].shape[0]), f32),
        ],
        name="adapter_grads",
    )(places, back_in, weighted, *x_pieces, *dy_pieces)


def local(
    tokens,
    cotangent,
    expert_choice,
    gate_values,
    gate_weight,
    up_weight,
    down_weight,
    shrinker,
    widener,
    squeezer,
    spreader,
):
    tok_rows, width = tokens.shape
    n_experts = lax.axis_size("dp")
    low_rank = spreader.shape[1]
    capacity = 80
    rows = n_experts * capacity
    me = lax.axis_index("expert")
    my_z, my_y = me // NY, me % NY

    flat_choice = expert_choice.reshape(-1)
    onehot = flat_choice[:, None] == jnp.arange(n_experts, dtype=jnp.int32)[None, :]
    n_flat = flat_choice.shape[0]
    order = jnp.arange(n_flat, dtype=jnp.int32)
    earlier = (order[None, :] < order[:, None]).astype(bf16)
    before = dot(earlier, onehot.astype(bf16), ((1,), (0,)))
    slot = jnp.sum(jnp.where(onehot, before, 0.0), axis=1).astype(jnp.int32)
    target = (flat_choice * capacity + slot).reshape(tok_rows, 2)
    places = jnp.arange(rows, dtype=jnp.int32)[:, None]
    hit_a = places == target[:, 0][None, :]
    hit_b = places == target[:, 1][None, :]
    pick_a, pick_b = hit_a.astype(bf16), hit_b.astype(bf16)
    both = jnp.concatenate([tokens, cotangent], axis=1)
    placed = dot(pick_a + pick_b, both, ((1,), (0,))).astype(bf16)
    gates = gate_values.astype(f32)
    send_gate = jnp.sum(
        jnp.where(hit_a, gates[:, 0][None, :], 0.0) + jnp.where(hit_b, gates[:, 1][None, :], 0.0),
        axis=1,
    ).astype(bf16)
    gate_block = jnp.pad(
        send_gate.reshape(n_experts, 1, capacity),
        ((0, 0), (0, GATE_ROWS - 1), (0, 2 * width - capacity)),
    )
    sent = jnp.concatenate([placed.reshape(n_experts, capacity, 2 * width), gate_block], axis=1)
    got = lax.all_to_all(sent, "dp", split_axis=0, concat_axis=0, tiled=True)
    gate_rows = got[:, capacity, :capacity].reshape(1, rows).astype(f32)
    first, second = turn(got, capacity)

    gate_w, up_w, down_w = gate_weight[0], up_weight[0], down_weight[0]
    shrink, widen, squeeze, spread = shrinker[0], widener[0], squeezer[0], spreader[0]
    hidden = gate_w.shape[1]
    gate_z = gate_w.reshape(NZ, NY * width, hidden)
    up_z = up_w.reshape(NZ, NY * width, hidden)
    shrink_z = shrink.reshape(2 * low_rank, NZ, NY * width).transpose(1, 0, 2)

    def by_y(w):
        return w.reshape(-1, NZ, NY, width).transpose(2, 0, 1, 3).reshape(NY, -1, NZ * width)

    down_y, spread_y = by_y(down_w), by_y(spread)

    group_x = jnp.zeros((NY, width, rows), bf16)
    for off, block in ring_gather(first, NY, shift_y):
        group_x = lax.dynamic_update_slice(group_x, block[None], ((my_y + off) % NY, 0, 0))
    group_dy = jnp.zeros((NZ, width, rows), bf16)
    for off, block in ring_gather(second, NZ, shift_z):
        group_dy = lax.dynamic_update_slice(group_dy, block[None], ((my_z + off) % NZ, 0, 0))
    x_pieces = ring_gather(group_x.reshape(NY * width, rows), NZ, shift_z)
    dy_pieces = ring_gather(group_dy.reshape(NZ * width, rows), NY, shift_y)
    x_places = jnp.stack([(my_z + off) % NZ for off, _ in x_pieces]).astype(jnp.int32)
    dy_places = jnp.stack([(my_y + off) % NY for off, _ in dy_pieces]).astype(jnp.int32)
    x_pieces = [piece for _, piece in x_pieces]
    dy_pieces = [piece for _, piece in dy_pieces]

    x_sums = early_x(x_places, x_pieces[:-1], gate_z, up_z, shrink_z)
    dy_sums = early_dy(dy_places, dy_pieces[:-1], down_y, spread_y)
    deltas, scaled_low, back_low, parts, widener_grad, squeezer_grad = middle(
        jnp.stack([x_places[-1], dy_places[-1]]),
        x_pieces[-1],
        dy_pieces[-1],
        gate_z,
        up_z,
        down_y,
        shrink_z,
        spread_y,
        widen,
        squeeze,
        gate_rows,
        *x_sums,
        *dy_sums,
    )
    gate_b = gate_w.reshape(NZ * NY, width, hidden)
    up_b = up_w.reshape(NZ * NY, width, hidden)
    term_y = input_term(gate_b, up_b, deltas, 0).reshape(NZ, NY, SPLIT_ROWS, rows)
    term_z = input_term(gate_b, up_b, deltas, 1).reshape(NZ, NY, width - SPLIT_ROWS, rows)

    def y_block(off):
        start = (my_y + off) % NY
        return lax.dynamic_index_in_dim(term_y, start, 1, keepdims=False).astype(f32)

    def z_block(off):
        start = (my_z + off) % NZ
        return lax.dynamic_index_in_dim(term_z, start, 0, keepdims=False).astype(f32)

    over_y = ring_reduce(y_block, NY, shift_y)
    steps = []
    over_z = ring_reduce(z_block, NZ, shift_z, steps)

    def then_z(off):
        return lax.dynamic_index_in_dim(over_y, (my_z + off) % NZ, 0, keepdims=False)

    def then_y(off):
        return lax.dynamic_index_in_dim(over_z, (my_y + off) % NY, 0, keepdims=False)

    sums = all_sum(parts, steps)
    back_in = sums[: 2 * low_rank].astype(bf16)
    out_low = sums[2 * low_rank : 3 * low_rank]
    gate_sum = sums[3 * low_rank : 3 * low_rank + 1]
    weighted_low = (out_low * gate_rows).astype(bf16)

    token_part = jnp.concatenate(
        [ring_reduce(then_z, NZ, shift_z), ring_reduce(then_y, NY, shift_y)], axis=0
    )
    shrink_cols = lax.dynamic_slice_in_dim(shrink, me * width, width, 1)
    token_part = token_part + adapter_scale * dot(shrink_cols, back_in, ((0,), (0,)))
    low_out = out_low.astype(bf16).astype(f32)
    gate_dots = gate_sum + adapter_scale * jnp.sum(low_out * back_low, axis=0, keepdims=True)

    returned = jnp.concatenate(
        [token_part.astype(bf16), jnp.pad(gate_dots, ((0, BACK_WIDTH - width - 1), (0, 0))).astype(bf16)],
        axis=0,
    )
    back = lax.all_to_all(
        returned.T.reshape(n_experts, capacity, BACK_WIDTH),
        "dp",
        split_axis=0,
        concat_axis=0,
        tiled=True,
    ).reshape(rows, BACK_WIDTH)
    part_a = dot(pick_a, back, ((0,), (0,)))
    part_b = dot(pick_b, back, ((0,), (0,)))
    token_grad = (part_a + part_b)[:, :width].astype(bf16)
    gate_grad = jnp.concatenate(
        [part_a[:, width : width + 1], part_b[:, width : width + 1]], axis=1
    )

    shrink_out, spread_out = adapter_grads(
        jnp.concatenate([x_places, dy_places]), x_pieces, dy_pieces, back_in, weighted_low
    )
    shrinker_grad = shrink_out.transpose(1, 0, 2).reshape(2 * low_rank, -1)
    spreader_grad = (
        spread_out.reshape(NY, low_rank, NZ, width).transpose(1, 2, 0, 3).reshape(low_rank, -1)
    )
    return (
        token_grad,
        gate_grad,
        shrinker_grad[None],
        widener_grad[None],
        squeezer_grad[None],
        spreader_grad[None],
    )


def solution(mesh):
    placed = (
        P("dp", "expert"),
        P("dp", "expert"),
        P("dp", None),
        P("dp", None),
        P("dp", None, "expert"),
        P("dp", None, "expert"),
        P("dp", "expert", None),
        P("dp", None, None),
        P("dp", None, None, "expert"),
        P("dp", None, "expert"),
        P("dp", None, None),
    )
    return jax.shard_map(
        local,
        mesh=mesh,
        in_specs=placed,
        out_specs=(
            P("dp", "expert"),
            P("dp", None),
            P("dp", None, None),
            P("dp", None, None, "expert"),
            P("dp", None, "expert"),
            P("dp", None, None),
        ),
        check_vma=False,
    )
```

```python
import jax
import jax.numpy as jnp
from jax import lax
from jax.experimental import pallas as pl
from jax.experimental.pallas import tpu as pltpu
from jax.sharding import PartitionSpec as P


adapter_scale = 2.0
NY = 4
NZ = 8
GATE_ROWS = 8
BACK_WIDTH = 256
SPLIT_ROWS = 96


bf16 = jnp.bfloat16
f32 = jnp.float32


def dot(a, b, dims):
    return lax.dot_general(a, b, (dims, ((), ())), preferred_element_type=f32)


def shift_y(x, d):
    pairs = [(z * NY + y, z * NY + (y + d) % NY) for z in range(NZ) for y in range(NY)]
    return lax.ppermute(x, "expert", pairs)


def shift_z(x, d):
    pairs = [(z * NY + y, (z + d) % NZ * NY + y) for z in range(NZ) for y in range(NY)]
    return lax.ppermute(x, "expert", pairs)


def hop(x, shift, d):
    return shift(x, d)


def far_pair(up, down, shift):
    half = up.shape[-2] // 32 * 16
    return jnp.concatenate(
        [hop(up[..., :half, :], shift, 1), hop(down[..., half:, :], shift, -1)],
        axis=-2,
    )


def ring_reduce(blocks, n, shift, seen=None):
    far = blocks(n // 2).astype(bf16)
    half = far.shape[-2] // 32 * 16
    up = hop(far[..., :half, :], shift, 1)
    down = hop(far[..., half:, :], shift, -1)
    if seen is not None:
        seen.append(up)
    lead = [(0, 0)] * (far.ndim - 2)
    rest = far.shape[-2] - half
    up = jnp.pad(up.astype(f32), lead + [(0, rest), (0, 0)])
    down = jnp.pad(down.astype(f32), lead + [(half, 0), (0, 0)])
    for k in range(n // 2 - 1, 0, -1):
        up = hop((up + blocks(k)).astype(bf16), shift, 1)
        down = hop((down + blocks(-k)).astype(bf16), shift, -1)
        if seen is not None:
            seen.append(up)
        up, down = up.astype(f32), down.astype(f32)
    return up + down + blocks(0)


def exchange(x, bit):
    pairs = [(e, e ^ bit) for e in range(NY * NZ)]
    x = x.astype(bf16)
    other = lax.ppermute(x, "expert", pairs)
    return x.astype(f32) + other.astype(f32)


def turn_kernel(got_ref, first_ref, second_ref, rows_ref):
    n, _, cols = got_ref.shape
    capacity = rows_ref.shape[0] // n
    for b in range(n):
        rows_ref[b * capacity : (b + 1) * capacity, :] = got_ref[b, :capacity, :]
    turned = rows_ref[...].T
    first_ref[...] = turned[: cols // 2]
    second_ref[...] = turned[cols // 2 :]


def turn(got, capacity):
    n, _, cols = got.shape
    rows = n * capacity
    return pl.pallas_call(
        turn_kernel,
        out_shape=(
            jax.ShapeDtypeStruct((cols // 2, rows), bf16),
            jax.ShapeDtypeStruct((cols // 2, rows), bf16),
        ),
        scratch_shapes=[pltpu.VMEM((rows, cols), bf16)],
        name="turn",
    )(got)


SMALL = pl.BlockSpec(memory_space=pltpu.SMEM)
BIG = pl.BlockSpec(memory_space=pltpu.VMEM)
FAR = pl.BlockSpec(memory_space=pl.ANY)


def accumulate(accs, values, start):
    for acc, value in zip(accs, values, strict=True):
        acc[...] = value if start else acc[...] + value


def early_x(places, pieces, gate_w, up_w, shrink, before=()):
    n, m = len(pieces), len(before)

    def kernel(places_ref, gate_w_ref, up_w_ref, shrink_ref, *refs):
        accs = refs[n + m : n + m + 3]
        weights_ref, sems = refs[n + m + 3 :]
        copies = [
            [
                pltpu.make_async_copy(src.at[places_ref[i]], weights_ref.at[j, i], sems.at[j, i])
                for j, src in enumerate((gate_w_ref, up_w_ref))
            ]
            for i in range(n)
        ]
        for pair in copies:
            for copy in pair:
                copy.start()
        if m:
            accumulate(accs, [ref[...] for ref in refs[n : n + m]], True)
        for i, ref in enumerate(refs[:n]):
            x = ref[...]
            for copy in copies[i]:
                copy.wait()
            values = (
                dot(weights_ref[0, i], x, ((0,), (0,))),
                dot(weights_ref[1, i], x, ((0,), (0,))),
                dot(shrink_ref[places_ref[i]], x, ((1,), (0,))),
            )
            accumulate(accs, values, i == 0 and not m)

    _, part, hidden = gate_w.shape
    n_rows = pieces[0].shape[1]
    return pl.pallas_call(
        kernel,
        in_specs=[SMALL, FAR, FAR] + [BIG] * (1 + n + m),
        out_specs=[BIG] * 3,
        out_shape=[
            jax.ShapeDtypeStruct((hidden, n_rows), f32),
            jax.ShapeDtypeStruct((hidden, n_rows), f32),
            jax.ShapeDtypeStruct((shrink.shape[1], n_rows), f32),
        ],
        scratch_shapes=[pltpu.VMEM((2, n, part, hidden), bf16), pltpu.SemaphoreType.DMA((2, n))],
        name="early_x",
    )(places, gate_w, up_w, shrink, *pieces, *before)


def early_dy(places, pieces, down_w, spread, before=()):
    n, m = len(pieces), len(before)
    count = sum(piece.shape[0] for piece in pieces)

    def kernel(places_ref, down_w_ref, spread_ref, *refs):
        accs = refs[n + m : n + m + 2]
        weights_ref, sems = refs[n + m + 2 :]
        copies = [
            pltpu.make_async_copy(down_w_ref.at[places_ref[i]], weights_ref.at[i], sems.at[i])
            for i in range(count)
        ]
        for copy in copies:
            copy.start()
        if m:
            accumulate(accs, [ref[...] for ref in refs[n : n + m]], True)
        at = 0
        for ref in refs[:n]:
            for j in range(ref.shape[0]):
                dy = ref[j]
                copies[at].wait()
                values = (
                    dot(weights_ref[at], dy, ((1,), (0,))),
                    dot(spread_ref[places_ref[at]], dy, ((1,), (0,))),
                )
                accumulate(accs, values, at == 0 and not m)
                at += 1

    _, hidden, width = down_w.shape
    n_rows = pieces[0].shape[2]
    return pl.pallas_call(
        kernel,
        in_specs=[SMALL, FAR] + [BIG] * (1 + n + m),
        out_specs=[BIG] * 2,
        out_shape=[
            jax.ShapeDtypeStruct((hidden, n_rows), f32),
            jax.ShapeDtypeStruct((spread.shape[1], n_rows), f32),
        ],
        scratch_shapes=[pltpu.VMEM((count, hidden, width), bf16), pltpu.SemaphoreType.DMA((count,))],
        name="early_dy",
    )(places, down_w, spread, *pieces, *before)


def middle_kernel(
    places_ref,
    lower_ref,
    upper_ref,
    gate_w_ref,
    up_w_ref,
    shrink_ref,
    widen_ref,
    squeeze_ref,
    gates_ref,
    gate_in_ref,
    up_in_ref,
    low_in_ref,
    down_in_ref,
    spread_in_ref,
    deltas_ref,
    scaled_ref,
    back_low_ref,
    parts_ref,
    widen_grad_ref,
    squeeze_grad_ref,
    weights_ref,
    sems,
):
    z = places_ref[0]
    copies = [
        pltpu.make_async_copy(src.at[z], weights_ref.at[j], sems.at[j])
        for j, src in enumerate((gate_w_ref, up_w_ref))
    ]
    for copy in copies:
        copy.start()
    lower, upper = lower_ref[...], upper_ref[...]
    rank, hidden = squeeze_ref.shape
    half, n_rows = lower.shape
    gates = gates_ref[...]
    squeeze = squeeze_ref[...]
    low = (
        low_in_ref[...]
        + dot(shrink_ref[z, :, :half], lower, ((1,), (0,)))
        + dot(shrink_ref[z, :, half:], upper, ((1,), (0,)))
    ).astype(bf16)
    back_low = spread_in_ref[...]
    back_low_ref[...] = back_low
    scaled = (back_low * gates).astype(bf16)
    scaled_ref[...] = scaled
    copies[0].wait()
    copies[1].wait()
    gate_pre = (
        gate_in_ref[...]
        + dot(weights_ref[0, :half], lower, ((0,), (0,)))
        + dot(weights_ref[0, half:], upper, ((0,), (0,)))
        + adapter_scale * dot(widen_ref[0], low[:rank], ((0,), (0,)))
    )
    up_pre = (
        up_in_ref[...]
        + dot(weights_ref[1, :half], lower, ((0,), (0,)))
        + dot(weights_ref[1, half:], upper, ((0,), (0,)))
        + adapter_scale * dot(widen_ref[1], low[rank:], ((0,), (0,)))
    )
    back_down = down_in_ref[...]
    logistic = jax.nn.sigmoid(gate_pre)
    silu_gate = gate_pre * logistic
    activation = (silu_gate * up_pre).astype(bf16)
    gate_part = jnp.sum(activation.astype(f32) * back_down, axis=0, keepdims=True)
    act_delta = gates * back_down + adapter_scale * dot(squeeze, scaled, ((0,), (0,)))
    slope = logistic * (1.0 + gate_pre * (1.0 - logistic))
    gate_delta = (act_delta * up_pre * slope).astype(bf16)
    up_delta = (act_delta * silu_gate).astype(bf16)
    deltas_ref[:hidden, :] = gate_delta
    deltas_ref[hidden:, :] = up_delta
    parts_ref[:rank, :] = dot(widen_ref[0], gate_delta, ((1,), (0,))).astype(bf16)
    parts_ref[rank : 2 * rank, :] = dot(widen_ref[1], up_delta, ((1,), (0,))).astype(bf16)
    parts_ref[2 * rank : 3 * rank, :] = dot(squeeze, activation, ((1,), (0,))).astype(bf16)
    parts_ref[3 * rank :, :] = jnp.broadcast_to(gate_part, (rank, n_rows)).astype(bf16)
    widen_grad_ref[0] = adapter_scale * dot(low[:rank], gate_delta, ((1,), (1,)))
    widen_grad_ref[1] = adapter_scale * dot(low[rank:], up_delta, ((1,), (1,)))
    squeeze_grad_ref[...] = adapter_scale * dot(scaled, activation, ((1,), (1,)))


def middle(places, lower, upper, gate_w, up_w, shrink, widen, squeeze, gates, *sums):
    rank, hidden = squeeze.shape
    n_rows = lower.shape[1]
    return pl.pallas_call(
        middle_kernel,
        in_specs=[SMALL] + [BIG] * 2 + [FAR] * 2 + [BIG] * 9,
        out_specs=[BIG] * 6,
        out_shape=[
            jax.ShapeDtypeStruct((2 * hidden, n_rows), bf16),
            jax.ShapeDtypeStruct((rank, n_rows), bf16),
            jax.ShapeDtypeStruct((rank, n_rows), f32),
            jax.ShapeDtypeStruct((4 * rank, n_rows), bf16),
            jax.ShapeDtypeStruct((2, rank, hidden), f32),
            jax.ShapeDtypeStruct((rank, hidden), f32),
        ],
        scratch_shapes=[
            pltpu.VMEM((2,) + gate_w.shape[1:], bf16),
            pltpu.SemaphoreType.DMA((2,)),
        ],
        name="middle",
    )(places, lower, upper, gate_w, up_w, shrink, widen, squeeze, gates, *sums)


def input_term(gate_w, up_w, deltas):
    n_blocks, width, hidden = gate_w.shape
    n_rows = deltas.shape[1]
    per = 4

    def kernel(gate_w_ref, up_w_ref, deltas_ref, first_ref, second_ref):
        weights = jnp.concatenate(
            [ref[...].reshape(per * width, hidden) for ref in (gate_w_ref, up_w_ref)], axis=1
        )
        total = dot(weights, deltas_ref[...], ((1,), (0,))).astype(bf16)
        total = total.reshape(per, width, n_rows)
        first_ref[...] = total[:, :SPLIT_ROWS]
        second_ref[...] = total[:, SPLIT_ROWS:]

    counts = (SPLIT_ROWS, width - SPLIT_ROWS)
    return pl.pallas_call(
        kernel,
        grid=(n_blocks // per,),
        in_specs=[
            pl.BlockSpec((per, width, hidden), lambda i: (i, 0, 0)),
            pl.BlockSpec((per, width, hidden), lambda i: (i, 0, 0)),
            pl.BlockSpec((2 * hidden, n_rows), lambda i: (0, 0)),
        ],
        out_specs=[pl.BlockSpec((per, count, n_rows), lambda i: (i, 0, 0)) for count in counts],
        out_shape=[jax.ShapeDtypeStruct((n_blocks, count, n_rows), bf16) for count in counts],
        name="input_term",
    )(gate_w, up_w, deltas)


def adapter_grads(x_places, x_pieces, x_halves, dy_places, dy_pieces, back_in, weighted):
    n_x, n_dy = len(x_pieces), len(dy_pieces)
    half = x_halves[0].shape[0]

    def kernel(x_places_ref, dy_places_ref, back_in_ref, weighted_ref, lower_ref, upper_ref, *refs):
        shrink_ref, spread_ref = refs[n_x + n_dy :]
        back = back_in_ref[...]
        for i, ref in enumerate(refs[:n_x]):
            shrink_ref[x_places_ref[i]] = adapter_scale * dot(back, ref[...], ((1,), (1,)))
        last = x_places_ref[n_x]
        shrink_ref[last, :, :half] = adapter_scale * dot(back, lower_ref[...], ((1,), (1,)))
        shrink_ref[last, :, half:] = adapter_scale * dot(back, upper_ref[...], ((1,), (1,)))
        at = 0
        for ref in refs[n_x : n_x + n_dy]:
            for j in range(ref.shape[0]):
                spread_ref[dy_places_ref[at]] = adapter_scale * dot(
                    weighted_ref[...], ref[j], ((1,), (1,))
                )
                at += 1

    return pl.pallas_call(
        kernel,
        in_specs=[SMALL] * 2 + [BIG] * (4 + n_x + n_dy),
        out_specs=[BIG] * 2,
        out_shape=[
            jax.ShapeDtypeStruct((NZ, back_in.shape[0], 2 * half), f32),
            jax.ShapeDtypeStruct((NZ * NY, weighted.shape[0], dy_pieces[0].shape[1]), f32),
        ],
        name="adapter_grads",
    )(x_places, dy_places, back_in, weighted, *x_halves, *x_pieces, *dy_pieces)


def whole_step(
    tokens,
    cotangent,
    expert_choice,
    gate_values,
    gate_weight,
    up_weight,
    down_weight,
    shrinker,
    widener,
    squeezer,
    spreader,
):
    tok_rows, width = tokens.shape
    n_experts = lax.axis_size("dp")
    low_rank = spreader.shape[1]
    capacity = 80
    rows = n_experts * capacity
    me = lax.axis_index("expert")
    my_z, my_y = me // NY, me % NY

    flat_choice = expert_choice.reshape(-1)
    onehot = flat_choice[:, None] == jnp.arange(n_experts, dtype=jnp.int32)[None, :]
    n_flat = flat_choice.shape[0]
    order = jnp.arange(n_flat, dtype=jnp.int32)
    earlier = (order[None, :] < order[:, None]).astype(bf16)
    before = dot(earlier, onehot.astype(bf16), ((1,), (0,)))
    slot = jnp.sum(jnp.where(onehot, before, 0.0), axis=1).astype(jnp.int32)
    target = (flat_choice * capacity + slot).reshape(tok_rows, 2)
    places = jnp.arange(rows, dtype=jnp.int32)[:, None]
    hit_a = places == target[:, 0][None, :]
    hit_b = places == target[:, 1][None, :]
    pick_a, pick_b = hit_a.astype(bf16), hit_b.astype(bf16)
    both = jnp.concatenate([tokens, cotangent], axis=1)
    placed = dot(pick_a + pick_b, both, ((1,), (0,))).astype(bf16)
    gates = gate_values.astype(f32)
    send_gate = jnp.sum(
        jnp.where(hit_a, gates[:, 0][None, :], 0.0) + jnp.where(hit_b, gates[:, 1][None, :], 0.0),
        axis=1,
    ).astype(bf16)
    gate_block = jnp.pad(
        send_gate.reshape(n_experts, 1, capacity),
        ((0, 0), (0, GATE_ROWS - 1), (0, 2 * width - capacity)),
    )
    sent = jnp.concatenate([placed.reshape(n_experts, capacity, 2 * width), gate_block], axis=1)
    got = lax.all_to_all(sent, "dp", split_axis=0, concat_axis=0, tiled=True)
    gate_w, up_w, down_w = gate_weight[0], up_weight[0], down_weight[0]
    shrink, widen, squeeze, spread = shrinker[0], widener[0], squeezer[0], spreader[0]
    hidden = gate_w.shape[1]
    gate_z = gate_w.reshape(NZ, NY * width, hidden)
    up_z = up_w.reshape(NZ, NY * width, hidden)
    shrink_z = shrink.reshape(2 * low_rank, NZ, NY * width).transpose(1, 0, 2)
    down_b = down_w.reshape(hidden, NZ * NY, width).transpose(1, 0, 2)
    spread_b = spread.reshape(low_rank, NZ * NY, width).transpose(1, 0, 2)
    got, shrink_z, down_b, spread_b = lax.optimization_barrier((got, shrink_z, down_b, spread_b))
    first, second = turn(got, capacity)
    gate_rows = got[:, capacity, :capacity].reshape(1, rows).astype(f32)

    up1, down1 = hop(second, shift_z, 1), hop(second, shift_z, -1)
    x_up, x_down = hop(first, shift_y, 1), hop(first, shift_y, -1)
    x_far = far_pair(x_up, x_down, shift_y)
    group_x = jnp.zeros((NY, width, rows), bf16)
    for off, block in ((0, first), (-1, x_up), (1, x_down), (2, x_far)):
        group_x = lax.dynamic_update_slice(group_x, block[None], ((my_y + off) % NY, 0, 0))
    group_x = group_x.reshape(NY * width, rows)
    up2, down2 = hop(up1, shift_z, 1), hop(down1, shift_z, -1)
    near = jnp.stack([second, up1, down1])
    up3, down3 = hop(up2, shift_z, 1), hop(down2, shift_z, -1)
    far = jnp.stack([up2, down2, up3, down3, far_pair(up3, down3, shift_z)])
    near_offs, far_offs = (0, -1, 1), (-2, 2, -3, 3, 4)

    near_up, near_down = hop(near, shift_y, 1), hop(near, shift_y, -1)
    near_far = far_pair(near_up, near_down, shift_y)
    far_up, far_down = hop(far, shift_y, 1), hop(far, shift_y, -1)
    far_far = (hop(far_up[:3], shift_y, 1), hop(far_down[3:], shift_y, -1))

    def places(z_offs, y_off):
        return [(my_z + z) % NZ * NY + (my_y + y_off) % NY for z in z_offs]

    dy_first = [near, near_up, near_down, far]
    dy_second = [near_far, far_up, far_down, far_far[0], far_far[1]]
    at_first = places(near_offs, 0) + places(near_offs, -1) + places(near_offs, 1) + places(far_offs, 0)
    at_second = (
        places(near_offs, 2)
        + places(far_offs, -1)
        + places(far_offs, 1)
        + places(far_offs[:3], 2)
        + places(far_offs[3:], 2)
    )
    at_first, at_second = jnp.stack(at_first), jnp.stack(at_second)

    x_up1, x_down1 = hop(group_x, shift_z, 1), hop(group_x, shift_z, -1)
    x_up2, x_down2 = hop(x_up1, shift_z, 1), hop(x_down1, shift_z, -1)
    x_up3, x_down3 = hop(x_up2, shift_z, 1), hop(x_down2, shift_z, -1)
    half = NY * width // 2
    lower, upper = hop(x_up3[:half], shift_z, 1), hop(x_down3[half:], shift_z, -1)
    x_all = [group_x, x_up1, x_down1, x_up2, x_down2, x_up3, x_down3]
    x_places = jnp.stack([(my_z + off) % NZ for off in (0, -1, 1, -2, 2, -3, 3, 4)])
    x_sums = early_x(x_places[:3], x_all[:3], gate_z, up_z, shrink_z)
    dy_sums = early_dy(at_first, dy_first, down_b, spread_b)
    dy_sums = early_dy(at_second, dy_second, down_b, spread_b, dy_sums)
    x_sums = early_x(x_places[3:5], x_all[3:5], gate_z, up_z, shrink_z, x_sums)
    x_sums = early_x(x_places[5:7], x_all[5:7], gate_z, up_z, shrink_z, x_sums)
    deltas, _, back_low, parts, widener_grad, squeezer_grad = middle(
        x_places[7:],
        lower,
        upper,
        gate_z,
        up_z,
        shrink_z,
        widen,
        squeeze,
        gate_rows,
        *x_sums,
        *dy_sums,
    )

    gate_b = gate_w.reshape(NZ * NY, width, hidden)
    up_b = up_w.reshape(NZ * NY, width, hidden)
    term_y, term_z = input_term(gate_b, up_b, deltas)
    term_z = term_z.reshape(NZ, NY, width - SPLIT_ROWS, rows)
    term_y = term_y.reshape(NZ, NY, SPLIT_ROWS, rows)

    def y_block(off):
        start = (my_y + off) % NY
        return lax.dynamic_index_in_dim(term_y, start, 1, keepdims=False).astype(f32)

    def z_block(off):
        start = (my_z + off) % NZ
        return lax.dynamic_index_in_dim(term_z, start, 0, keepdims=False).astype(f32)

    over_z = ring_reduce(z_block, NZ, shift_z)
    over_y = ring_reduce(y_block, NY, shift_y)

    sums = parts
    for bit in (1, 2, 4, 8, 16):
        sums = exchange(sums, bit)
    back_in = sums[: 2 * low_rank].astype(bf16)
    out_low = sums[2 * low_rank : 3 * low_rank]
    gate_sum = sums[3 * low_rank : 3 * low_rank + 1]
    weighted_low = (out_low * gate_rows).astype(bf16)
    shrink_out, spread_out = adapter_grads(
        x_places,
        x_all,
        (lower, upper),
        jnp.concatenate([at_first, at_second]),
        dy_first + dy_second,
        back_in,
        weighted_low,
    )
    shrinker_grad = shrink_out.transpose(1, 0, 2).reshape(2 * low_rank, -1)
    spreader_grad = spread_out.transpose(1, 0, 2).reshape(low_rank, -1)

    def then_z(off):
        return lax.dynamic_index_in_dim(over_y, (my_z + off) % NZ, 0, keepdims=False)

    def then_y(off):
        return lax.dynamic_index_in_dim(over_z, (my_y + off) % NY, 0, keepdims=False)

    token_part = jnp.concatenate(
        [ring_reduce(then_z, NZ, shift_z), ring_reduce(then_y, NY, shift_y)], axis=0
    )
    shrink_cols = lax.dynamic_slice_in_dim(shrink, me * width, width, 1)
    token_part = token_part + adapter_scale * dot(shrink_cols, back_in, ((0,), (0,)))
    low_out = out_low.astype(bf16).astype(f32)
    gate_dots = gate_sum + adapter_scale * jnp.sum(low_out * back_low, axis=0, keepdims=True)

    returned = jnp.concatenate(
        [token_part.astype(bf16), jnp.pad(gate_dots, ((0, BACK_WIDTH - width - 1), (0, 0))).astype(bf16)],
        axis=0,
    )
    returned = returned.T.reshape(n_experts, capacity, BACK_WIDTH)
    back = lax.all_to_all(returned, "dp", split_axis=0, concat_axis=0, tiled=True)
    back = back.reshape(rows, BACK_WIDTH)
    part_a = dot(pick_a, back, ((0,), (0,)))
    part_b = dot(pick_b, back, ((0,), (0,)))
    token_grad = (part_a + part_b)[:, :width].astype(bf16)
    gate_grad = jnp.concatenate(
        [part_a[:, width : width + 1], part_b[:, width : width + 1]], axis=1
    )

    return (
        token_grad,
        gate_grad,
        shrinker_grad[None],
        widener_grad[None],
        squeezer_grad[None],
        spreader_grad[None],
    )


def solution(mesh):
    placed = (
        P("dp", "expert"),
        P("dp", "expert"),
        P("dp", None),
        P("dp", None),
        P("dp", None, "expert"),
        P("dp", None, "expert"),
        P("dp", "expert", None),
        P("dp", None, None),
        P("dp", None, None, "expert"),
        P("dp", None, "expert"),
        P("dp", None, None),
    )
    return jax.shard_map(
        whole_step,
        mesh=mesh,
        in_specs=placed,
        out_specs=(
            P("dp", "expert"),
            P("dp", None),
            P("dp", None, None),
            P("dp", None, None, "expert"),
            P("dp", None, "expert"),
            P("dp", None, None),
        ),
        check_vma=False,
    )
```

```python
import jax
import jax.numpy as jnp
from jax import lax
from jax.experimental import pallas as pl
from jax.experimental.pallas import tpu as pltpu
from jax.sharding import PartitionSpec as P


adapter_scale = 2.0
NY = 4
NZ = 8
GATE_ROWS = 8
BACK_WIDTH = 256
SPLIT_ROWS = 96


bf16 = jnp.bfloat16
f32 = jnp.float32


def dot(a, b, dims):
    return lax.dot_general(a, b, (dims, ((), ())), preferred_element_type=f32)


def shift_y(x, d):
    pairs = [(z * NY + y, z * NY + (y + d) % NY) for z in range(NZ) for y in range(NY)]
    return lax.ppermute(x, "expert", pairs)


def shift_z(x, d):
    pairs = [(z * NY + y, (z + d) % NZ * NY + y) for z in range(NZ) for y in range(NY)]
    return lax.ppermute(x, "expert", pairs)


def hop(x, shift, d):
    return shift(x, d)


def far_pair(up, down, shift):
    half = up.shape[-2] // 32 * 16
    return jnp.concatenate(
        [hop(up[..., :half, :], shift, 1), hop(down[..., half:, :], shift, -1)],
        axis=-2,
    )


def ring_reduce(blocks, n, shift, seen=None):
    far = blocks(n // 2).astype(bf16)
    half = far.shape[-2] // 32 * 16
    up = hop(far[..., :half, :], shift, 1)
    down = hop(far[..., half:, :], shift, -1)
    if seen is not None:
        seen.append(up)
    lead = [(0, 0)] * (far.ndim - 2)
    rest = far.shape[-2] - half
    up = jnp.pad(up.astype(f32), lead + [(0, rest), (0, 0)])
    down = jnp.pad(down.astype(f32), lead + [(half, 0), (0, 0)])
    for k in range(n // 2 - 1, 0, -1):
        up = hop((up + blocks(k)).astype(bf16), shift, 1)
        down = hop((down + blocks(-k)).astype(bf16), shift, -1)
        if seen is not None:
            seen.append(up)
        up, down = up.astype(f32), down.astype(f32)
    return up + down + blocks(0)


def exchange(x, bit):
    pairs = [(e, e ^ bit) for e in range(NY * NZ)]
    x = x.astype(bf16)
    other = lax.ppermute(x, "expert", pairs)
    return x.astype(f32) + other.astype(f32)


def turn_kernel(got_ref, first_ref, second_ref, rows_ref):
    n, _, cols = got_ref.shape
    capacity = rows_ref.shape[0] // n
    for b in range(n):
        rows_ref[b * capacity : (b + 1) * capacity, :] = got_ref[b, :capacity, :]
    turned = rows_ref[...].T
    first_ref[...] = turned[: cols // 2]
    second_ref[...] = turned[cols // 2 :]


def turn(got, capacity):
    n, _, cols = got.shape
    rows = n * capacity
    return pl.pallas_call(
        turn_kernel,
        out_shape=(
            jax.ShapeDtypeStruct((cols // 2, rows), bf16),
            jax.ShapeDtypeStruct((cols // 2, rows), bf16),
        ),
        scratch_shapes=[pltpu.VMEM((rows, cols), bf16)],
        name="turn",
    )(got)


SMALL = pl.BlockSpec(memory_space=pltpu.SMEM)
BIG = pl.BlockSpec(memory_space=pltpu.VMEM)
FAR = pl.BlockSpec(memory_space=pl.ANY)


def accumulate(accs, values, start):
    for acc, value in zip(accs, values, strict=True):
        acc[...] = value if start else acc[...] + value


def early_x(places, pieces, gate_w, up_w, shrink, before=()):
    n, m = len(pieces), len(before)

    def kernel(places_ref, gate_w_ref, up_w_ref, shrink_ref, *refs):
        accs = refs[n + m : n + m + 3]
        weights_ref, sems = refs[n + m + 3 :]
        copies = [
            [
                pltpu.make_async_copy(src.at[places_ref[i]], weights_ref.at[j, i], sems.at[j, i])
                for j, src in enumerate((gate_w_ref, up_w_ref))
            ]
            for i in range(n)
        ]
        for pair in copies:
            for copy in pair:
                copy.start()
        if m:
            accumulate(accs, [ref[...] for ref in refs[n : n + m]], True)
        for i, ref in enumerate(refs[:n]):
            x = ref[...]
            for copy in copies[i]:
                copy.wait()
            values = (
                dot(weights_ref[0, i], x, ((0,), (0,))),
                dot(weights_ref[1, i], x, ((0,), (0,))),
                dot(shrink_ref[places_ref[i]], x, ((1,), (0,))),
            )
            accumulate(accs, values, i == 0 and not m)

    _, part, hidden = gate_w.shape
    n_rows = pieces[0].shape[1]
    return pl.pallas_call(
        kernel,
        in_specs=[SMALL, FAR, FAR] + [BIG] * (1 + n + m),
        out_specs=[BIG] * 3,
        out_shape=[
            jax.ShapeDtypeStruct((hidden, n_rows), f32),
            jax.ShapeDtypeStruct((hidden, n_rows), f32),
            jax.ShapeDtypeStruct((shrink.shape[1], n_rows), f32),
        ],
        scratch_shapes=[pltpu.VMEM((2, n, part, hidden), bf16), pltpu.SemaphoreType.DMA((2, n))],
        name="early_x",
    )(places, gate_w, up_w, shrink, *pieces, *before)


def early_dy(places, pieces, down_w, spread, before=()):
    n, m = len(pieces), len(before)
    count = sum(piece.shape[0] for piece in pieces)

    def kernel(places_ref, down_w_ref, spread_ref, *refs):
        accs = refs[n + m : n + m + 2]
        weights_ref, sems = refs[n + m + 2 :]
        copies = [
            pltpu.make_async_copy(down_w_ref.at[places_ref[i]], weights_ref.at[i], sems.at[i])
            for i in range(count)
        ]
        for copy in copies:
            copy.start()
        if m:
            accumulate(accs, [ref[...] for ref in refs[n : n + m]], True)
        at = 0
        for ref in refs[:n]:
            for j in range(ref.shape[0]):
                dy = ref[j]
                copies[at].wait()
                values = (
                    dot(weights_ref[at], dy, ((1,), (0,))),
                    dot(spread_ref[places_ref[at]], dy, ((1,), (0,))),
                )
                accumulate(accs, values, at == 0 and not m)
                at += 1

    _, hidden, width = down_w.shape
    n_rows = pieces[0].shape[2]
    return pl.pallas_call(
        kernel,
        in_specs=[SMALL, FAR] + [BIG] * (1 + n + m),
        out_specs=[BIG] * 2,
        out_shape=[
            jax.ShapeDtypeStruct((hidden, n_rows), f32),
            jax.ShapeDtypeStruct((spread.shape[1], n_rows), f32),
        ],
        scratch_shapes=[pltpu.VMEM((count, hidden, width), bf16), pltpu.SemaphoreType.DMA((count,))],
        name="early_dy",
    )(places, down_w, spread, *pieces, *before)


def middle_kernel(
    places_ref,
    lower_ref,
    upper_ref,
    gate_w_ref,
    up_w_ref,
    shrink_ref,
    widen_ref,
    squeeze_ref,
    gates_ref,
    gate_in_ref,
    up_in_ref,
    low_in_ref,
    down_in_ref,
    spread_in_ref,
    deltas_ref,
    scaled_ref,
    back_low_ref,
    parts_ref,
    widen_grad_ref,
    squeeze_grad_ref,
    weights_ref,
    sems,
):
    z = places_ref[0]
    copies = [
        pltpu.make_async_copy(src.at[z], weights_ref.at[j], sems.at[j])
        for j, src in enumerate((gate_w_ref, up_w_ref))
    ]
    for copy in copies:
        copy.start()
    lower, upper = lower_ref[...], upper_ref[...]
    rank, hidden = squeeze_ref.shape
    half, n_rows = lower.shape
    gates = gates_ref[...]
    squeeze = squeeze_ref[...]
    low = (
        low_in_ref[...]
        + dot(shrink_ref[z, :, :half], lower, ((1,), (0,)))
        + dot(shrink_ref[z, :, half:], upper, ((1,), (0,)))
    ).astype(bf16)
    back_low = spread_in_ref[...]
    back_low_ref[...] = back_low
    scaled = (back_low * gates).astype(bf16)
    scaled_ref[...] = scaled
    copies[0].wait()
    copies[1].wait()
    gate_pre = (
        gate_in_ref[...]
        + dot(weights_ref[0, :half], lower, ((0,), (0,)))
        + dot(weights_ref[0, half:], upper, ((0,), (0,)))
        + adapter_scale * dot(widen_ref[0], low[:rank], ((0,), (0,)))
    )
    up_pre = (
        up_in_ref[...]
        + dot(weights_ref[1, :half], lower, ((0,), (0,)))
        + dot(weights_ref[1, half:], upper, ((0,), (0,)))
        + adapter_scale * dot(widen_ref[1], low[rank:], ((0,), (0,)))
    )
    back_down = down_in_ref[...]
    logistic = jax.nn.sigmoid(gate_pre)
    silu_gate = gate_pre * logistic
    activation = (silu_gate * up_pre).astype(bf16)
    gate_part = jnp.sum(activation.astype(f32) * back_down, axis=0, keepdims=True)
    act_delta = gates * back_down + adapter_scale * dot(squeeze, scaled, ((0,), (0,)))
    slope = logistic * (1.0 + gate_pre * (1.0 - logistic))
    gate_delta = (act_delta * up_pre * slope).astype(bf16)
    up_delta = (act_delta * silu_gate).astype(bf16)
    deltas_ref[:hidden, :] = gate_delta
    deltas_ref[hidden:, :] = up_delta
    parts_ref[:rank, :] = dot(widen_ref[0], gate_delta, ((1,), (0,))).astype(bf16)
    parts_ref[rank : 2 * rank, :] = dot(widen_ref[1], up_delta, ((1,), (0,))).astype(bf16)
    parts_ref[2 * rank : 3 * rank, :] = dot(squeeze, activation, ((1,), (0,))).astype(bf16)
    parts_ref[3 * rank :, :] = jnp.broadcast_to(gate_part, (rank, n_rows)).astype(bf16)
    widen_grad_ref[0] = adapter_scale * dot(low[:rank], gate_delta, ((1,), (1,)))
    widen_grad_ref[1] = adapter_scale * dot(low[rank:], up_delta, ((1,), (1,)))
    squeeze_grad_ref[...] = adapter_scale * dot(scaled, activation, ((1,), (1,)))


def middle(places, lower, upper, gate_w, up_w, shrink, widen, squeeze, gates, *sums):
    rank, hidden = squeeze.shape
    n_rows = lower.shape[1]
    return pl.pallas_call(
        middle_kernel,
        in_specs=[SMALL] + [BIG] * 2 + [FAR] * 2 + [BIG] * 9,
        out_specs=[BIG] * 6,
        out_shape=[
            jax.ShapeDtypeStruct((2 * hidden, n_rows), bf16),
            jax.ShapeDtypeStruct((rank, n_rows), bf16),
            jax.ShapeDtypeStruct((rank, n_rows), f32),
            jax.ShapeDtypeStruct((4 * rank, n_rows), bf16),
            jax.ShapeDtypeStruct((2, rank, hidden), f32),
            jax.ShapeDtypeStruct((rank, hidden), f32),
        ],
        scratch_shapes=[
            pltpu.VMEM((2,) + gate_w.shape[1:], bf16),
            pltpu.SemaphoreType.DMA((2,)),
        ],
        name="middle",
    )(places, lower, upper, gate_w, up_w, shrink, widen, squeeze, gates, *sums)


def input_term(gate_w, up_w, deltas):
    n_blocks, width, hidden = gate_w.shape
    n_rows = deltas.shape[1]
    per = 4

    def kernel(gate_w_ref, up_w_ref, deltas_ref, first_ref, second_ref):
        weights = jnp.concatenate(
            [ref[...].reshape(per * width, hidden) for ref in (gate_w_ref, up_w_ref)], axis=1
        )
        total = dot(weights, deltas_ref[...], ((1,), (0,))).astype(bf16)
        total = total.reshape(per, width, n_rows)
        first_ref[...] = total[:, :SPLIT_ROWS]
        second_ref[...] = total[:, SPLIT_ROWS:]

    counts = (SPLIT_ROWS, width - SPLIT_ROWS)
    return pl.pallas_call(
        kernel,
        grid=(n_blocks // per,),
        in_specs=[
            pl.BlockSpec((per, width, hidden), lambda i: (i, 0, 0)),
            pl.BlockSpec((per, width, hidden), lambda i: (i, 0, 0)),
            pl.BlockSpec((2 * hidden, n_rows), lambda i: (0, 0)),
        ],
        out_specs=[pl.BlockSpec((per, count, n_rows), lambda i: (i, 0, 0)) for count in counts],
        out_shape=[jax.ShapeDtypeStruct((n_blocks, count, n_rows), bf16) for count in counts],
        name="input_term",
    )(gate_w, up_w, deltas)


def shrinker_blocks(places, pieces, halves, back_in):
    n, half = len(pieces), halves[0].shape[0]

    def kernel(places_ref, back_in_ref, lower_ref, upper_ref, *refs):
        out_ref, back = refs[n], back_in_ref[...]
        for i, ref in enumerate(refs[:n]):
            out_ref[places_ref[i]] = adapter_scale * dot(back, ref[...], ((1,), (1,)))
        last = places_ref[n]
        out_ref[last, :, :half] = adapter_scale * dot(back, lower_ref[...], ((1,), (1,)))
        out_ref[last, :, half:] = adapter_scale * dot(back, upper_ref[...], ((1,), (1,)))

    return pl.pallas_call(
        kernel,
        in_specs=[SMALL] + [BIG] * (3 + n),
        out_specs=BIG,
        out_shape=jax.ShapeDtypeStruct((NZ, back_in.shape[0], 2 * half), f32),
        name="shrinker_blocks",
    )(places, back_in, *halves, *pieces)


def spreader_blocks(places, pieces, weighted):
    n = len(pieces)

    def kernel(places_ref, weighted_ref, *refs):
        out_ref, weights = refs[n], weighted_ref[...]
        at = 0
        for ref in refs[:n]:
            for j in range(ref.shape[0]):
                out_ref[places_ref[at]] = adapter_scale * dot(weights, ref[j], ((1,), (1,)))
                at += 1

    return pl.pallas_call(
        kernel,
        in_specs=[SMALL] + [BIG] * (1 + n),
        out_specs=BIG,
        out_shape=jax.ShapeDtypeStruct((NZ * NY, weighted.shape[0], pieces[0].shape[1]), f32),
        name="spreader_blocks",
    )(places, weighted, *pieces)


def whole_step(
    tokens,
    cotangent,
    expert_choice,
    gate_values,
    gate_weight,
    up_weight,
    down_weight,
    shrinker,
    widener,
    squeezer,
    spreader,
):
    tok_rows, width = tokens.shape
    n_experts = lax.axis_size("dp")
    low_rank = spreader.shape[1]
    capacity = 80
    rows = n_experts * capacity
    me = lax.axis_index("expert")
    my_z, my_y = me // NY, me % NY

    flat_choice = expert_choice.reshape(-1)
    onehot = flat_choice[:, None] == jnp.arange(n_experts, dtype=jnp.int32)[None, :]
    n_flat = flat_choice.shape[0]
    order = jnp.arange(n_flat, dtype=jnp.int32)
    earlier = (order[None, :] < order[:, None]).astype(bf16)
    before = dot(earlier, onehot.astype(bf16), ((1,), (0,)))
    slot = jnp.sum(jnp.where(onehot, before, 0.0), axis=1).astype(jnp.int32)
    target = (flat_choice * capacity + slot).reshape(tok_rows, 2)
    places = jnp.arange(rows, dtype=jnp.int32)[:, None]
    hit_a = places == target[:, 0][None, :]
    hit_b = places == target[:, 1][None, :]
    pick_a, pick_b = hit_a.astype(bf16), hit_b.astype(bf16)
    both = jnp.concatenate([tokens, cotangent], axis=1)
    placed = dot(pick_a + pick_b, both, ((1,), (0,))).astype(bf16)
    gates = gate_values.astype(f32)
    send_gate = jnp.sum(
        jnp.where(hit_a, gates[:, 0][None, :], 0.0) + jnp.where(hit_b, gates[:, 1][None, :], 0.0),
        axis=1,
    ).astype(bf16)
    gate_block = jnp.pad(
        send_gate.reshape(n_experts, 1, capacity),
        ((0, 0), (0, GATE_ROWS - 1), (0, 2 * width - capacity)),
    )
    sent = jnp.concatenate([placed.reshape(n_experts, capacity, 2 * width), gate_block], axis=1)
    got = lax.all_to_all(sent, "dp", split_axis=0, concat_axis=0, tiled=True)
    gate_w, up_w, down_w = gate_weight[0], up_weight[0], down_weight[0]
    shrink, widen, squeeze, spread = shrinker[0], widener[0], squeezer[0], spreader[0]
    hidden = gate_w.shape[1]
    gate_z = gate_w.reshape(NZ, NY * width, hidden)
    up_z = up_w.reshape(NZ, NY * width, hidden)
    shrink_z = shrink.reshape(2 * low_rank, NZ, NY * width).transpose(1, 0, 2)
    down_b = down_w.reshape(hidden, NZ * NY, width).transpose(1, 0, 2)
    spread_b = spread.reshape(low_rank, NZ * NY, width).transpose(1, 0, 2)
    got, shrink_z, down_b, spread_b = lax.optimization_barrier((got, shrink_z, down_b, spread_b))
    first, second = turn(got, capacity)
    gate_rows = got[:, capacity, :capacity].reshape(1, rows).astype(f32)

    up1, down1 = hop(second, shift_z, 1), hop(second, shift_z, -1)
    x_up, x_down = hop(first, shift_y, 1), hop(first, shift_y, -1)
    x_far = far_pair(x_up, x_down, shift_y)
    group_x = jnp.zeros((NY, width, rows), bf16)
    for off, block in ((0, first), (-1, x_up), (1, x_down), (2, x_far)):
        group_x = lax.dynamic_update_slice(group_x, block[None], ((my_y + off) % NY, 0, 0))
    group_x = group_x.reshape(NY * width, rows)
    up2, down2 = hop(up1, shift_z, 1), hop(down1, shift_z, -1)
    near = jnp.stack([second, up1, down1])
    up3, down3 = hop(up2, shift_z, 1), hop(down2, shift_z, -1)
    far = jnp.stack([up2, down2, up3, down3, far_pair(up3, down3, shift_z)])
    near_offs, far_offs = (0, -1, 1), (-2, 2, -3, 3, 4)

    near_up, near_down = hop(near, shift_y, 1), hop(near, shift_y, -1)
    near_far = far_pair(near_up, near_down, shift_y)
    far_up, far_down = hop(far, shift_y, 1), hop(far, shift_y, -1)
    far_far = (hop(far_up[:3], shift_y, 1), hop(far_down[3:], shift_y, -1))

    def places(z_offs, y_off):
        return [(my_z + z) % NZ * NY + (my_y + y_off) % NY for z in z_offs]

    dy_first = [near, near_up, near_down, far]
    dy_second = [near_far, far_up, far_down, far_far[0], far_far[1]]
    at_first = places(near_offs, 0) + places(near_offs, -1) + places(near_offs, 1) + places(far_offs, 0)
    at_second = (
        places(near_offs, 2)
        + places(far_offs, -1)
        + places(far_offs, 1)
        + places(far_offs[:3], 2)
        + places(far_offs[3:], 2)
    )
    at_first, at_second = jnp.stack(at_first), jnp.stack(at_second)

    x_up1, x_down1 = hop(group_x, shift_z, 1), hop(group_x, shift_z, -1)
    x_up2, x_down2 = hop(x_up1, shift_z, 1), hop(x_down1, shift_z, -1)
    x_up3, x_down3 = hop(x_up2, shift_z, 1), hop(x_down2, shift_z, -1)
    half = NY * width // 2
    lower, upper = hop(x_up3[:half], shift_z, 1), hop(x_down3[half:], shift_z, -1)
    x_all = [group_x, x_up1, x_down1, x_up2, x_down2, x_up3, x_down3]
    x_places = jnp.stack([(my_z + off) % NZ for off in (0, -1, 1, -2, 2, -3, 3, 4)])
    x_sums = early_x(x_places[:3], x_all[:3], gate_z, up_z, shrink_z)
    dy_sums = early_dy(at_first, dy_first, down_b, spread_b)
    dy_sums = early_dy(at_second, dy_second, down_b, spread_b, dy_sums)
    x_sums = early_x(x_places[3:5], x_all[3:5], gate_z, up_z, shrink_z, x_sums)
    x_sums = early_x(x_places[5:7], x_all[5:7], gate_z, up_z, shrink_z, x_sums)
    deltas, _, back_low, parts, widener_grad, squeezer_grad = middle(
        x_places[7:],
        lower,
        upper,
        gate_z,
        up_z,
        shrink_z,
        widen,
        squeeze,
        gate_rows,
        *x_sums,
        *dy_sums,
    )

    gate_b = gate_w.reshape(NZ * NY, width, hidden)
    up_b = up_w.reshape(NZ * NY, width, hidden)
    term_y, term_z = input_term(gate_b, up_b, deltas)
    term_z = term_z.reshape(NZ, NY, width - SPLIT_ROWS, rows)
    term_y = term_y.reshape(NZ, NY, SPLIT_ROWS, rows)

    def y_block(off):
        start = (my_y + off) % NY
        return lax.dynamic_index_in_dim(term_y, start, 1, keepdims=False).astype(f32)

    def z_block(off):
        start = (my_z + off) % NZ
        return lax.dynamic_index_in_dim(term_z, start, 0, keepdims=False).astype(f32)

    over_z = ring_reduce(z_block, NZ, shift_z)
    over_y = ring_reduce(y_block, NY, shift_y)

    sums = parts
    for bit in (1, 2, 4, 8, 16):
        sums = exchange(sums, bit)
    back_in = sums[: 2 * low_rank].astype(bf16)
    out_low = sums[2 * low_rank : 3 * low_rank]
    gate_sum = sums[3 * low_rank : 3 * low_rank + 1]
    weighted_low = (out_low * gate_rows).astype(bf16)
    shrink_out = shrinker_blocks(x_places, x_all, (lower, upper), back_in)
    spread_out = spreader_blocks(
        jnp.concatenate([at_first, at_second]), dy_first + dy_second, weighted_low
    )
    shrinker_grad = shrink_out.transpose(1, 0, 2).reshape(2 * low_rank, -1)
    spreader_grad = spread_out.transpose(1, 0, 2).reshape(low_rank, -1)

    def then_z(off):
        return lax.dynamic_index_in_dim(over_y, (my_z + off) % NZ, 0, keepdims=False)

    def then_y(off):
        return lax.dynamic_index_in_dim(over_z, (my_y + off) % NY, 0, keepdims=False)

    token_part = jnp.concatenate(
        [ring_reduce(then_z, NZ, shift_z), ring_reduce(then_y, NY, shift_y)], axis=0
    )
    shrink_cols = lax.dynamic_slice_in_dim(shrink, me * width, width, 1)
    token_part = token_part + adapter_scale * dot(shrink_cols, back_in, ((0,), (0,)))
    low_out = out_low.astype(bf16).astype(f32)
    gate_dots = gate_sum + adapter_scale * jnp.sum(low_out * back_low, axis=0, keepdims=True)

    returned = jnp.concatenate(
        [token_part.astype(bf16), jnp.pad(gate_dots, ((0, BACK_WIDTH - width - 1), (0, 0))).astype(bf16)],
        axis=0,
    )
    returned = returned.T.reshape(n_experts, capacity, BACK_WIDTH)
    back = lax.all_to_all(returned, "dp", split_axis=0, concat_axis=0, tiled=True)
    back = back.reshape(rows, BACK_WIDTH)
    part_a = dot(pick_a, back, ((0,), (0,)))
    part_b = dot(pick_b, back, ((0,), (0,)))
    token_grad = (part_a + part_b)[:, :width].astype(bf16)
    gate_grad = jnp.concatenate(
        [part_a[:, width : width + 1], part_b[:, width : width + 1]], axis=1
    )

    return (
        token_grad,
        gate_grad,
        shrinker_grad[None],
        widener_grad[None],
        squeezer_grad[None],
        spreader_grad[None],
    )


def solution(mesh):
    placed = (
        P("dp", "expert"),
        P("dp", "expert"),
        P("dp", None),
        P("dp", None),
        P("dp", None, "expert"),
        P("dp", None, "expert"),
        P("dp", "expert", None),
        P("dp", None, None),
        P("dp", None, None, "expert"),
        P("dp", None, "expert"),
        P("dp", None, None),
    )
    return jax.shard_map(
        whole_step,
        mesh=mesh,
        in_specs=placed,
        out_specs=(
            P("dp", "expert"),
            P("dp", None),
            P("dp", None, None),
            P("dp", None, None, "expert"),
            P("dp", None, "expert"),
            P("dp", None, None),
        ),
        check_vma=False,
    )
```
